32 devices in a mesh: prow: 8 (over z, x), pcol: 4 (over y, core).
Axes of the slice: x: 2, y: 2, z: 4, core: 2. Of those that a mesh axis runs over, the one named last changes fastest.
Arguments:
- a_matrix: bfloat16 [32768, 512], P('prow', 'pcol'), may hold values from -6 to 6
- l_panel: bfloat16 [32768, 256], P('prow', 'pcol'), may hold values from -0.375 to 0.375
- l_inverse: bfloat16 [256, 256], replicated, may hold values from -1 to 1
- pivots: int32 [256], replicated, may hold values from 0 to 32767, as said below
Outputs:
- updated: bfloat16 [32768, 512], P('prow', 'pcol')
The draws below stay inside these ranges and needn't reach their ends.
Inputs may be any that keep to these rules, and one draw needn't show every extreme that they name: pivots[j] >= j for every j.
All inputs are finite; a program needn't handle non-finite values.
Results may differ from the reference program's by a relative error of at most 0.0039.
Values may be sent and summed in bfloat16 or wider, within the bound.
A program may use at most 64 MiB of HBM per device.

```python
import math
import jax
import jax.numpy as jnp
from jax import lax

N = 32768
NB = 256
ROWS_DEV = 4096
WIDTH = 512
N_PROW = 8


def draw_l_inverse(key, part):
    sub_key = jax.random.fold_in(key, 11)
    spread_scale = 0.6 / math.sqrt(NB)
    entries = jnp.clip(jax.random.normal(sub_key, (NB, NB), jnp.float32), -4.0, 4.0) * spread_scale
    triangle = jnp.tril(entries, -1) + jnp.eye(NB, dtype=jnp.float32)
    return triangle.astype(jnp.bfloat16)


def draw_pivots(key, part):
    sub_key = jax.random.fold_in(key, 7)
    starts = jnp.arange(NB, dtype=jnp.int32)
    offsets = jax.random.randint(sub_key, (NB,), 0, N - starts, dtype=jnp.int32)
    chosen = starts + offsets
    chosen = chosen.at[0].set(0)
    return chosen.at[NB - 1].set(N - 1)


def shard_levels(rng, shape, shards, low, high):
    gain, own = 1.0, jax.random.fold_in(rng, 6)
    for position, parts in shards:
        steps = jnp.exp(jax.random.uniform(jax.random.fold_in(own, position), (parts,), jnp.float32, low / len(shards), high / len(shards)))
        gain = gain * jnp.repeat(steps, shape[position] // parts).reshape([-1 if axis == position else 1 for axis in range(len(shape))])
    return gain


def noise(rng, dims, deviation, reach, shards=(), held_as=jnp.bfloat16):
    array = deviation * jax.random.normal(rng, dims, jnp.float32)
    if shards:
        array = array * shard_levels(rng, dims, shards, -0.22, 0.18)
    return jnp.clip(array, -reach, reach).astype(held_as)


def setup_inputs(seed: int = 0) -> dict:
    arg_keys = jax.random.split(jax.random.key(seed), 5)
    return {
        "a_matrix": noise(arg_keys[0], (N, WIDTH), 1.0, 6.0, ((0, 8), (1, 4))),
        "l_panel": noise(arg_keys[1], (N, NB), NB ** -0.5, 0.375, ((0, 8), (1, 4))),
        "l_inverse": draw_l_inverse(jax.random.fold_in(arg_keys[4], 71), 0),
        "pivots": draw_pivots(jax.random.fold_in(arg_keys[4], 71), 0),
    }


def swap_plan(pivots, panel_width):
    slot_ids = jnp.arange(panel_width, dtype=jnp.int32)
    earlier = slot_ids[None, :] < slot_ids[:, None]
    hits = (pivots[None, :] == slot_ids[:, None]) & earlier
    pointer = jnp.max(jnp.where(hits, slot_ids[None, :], -1), axis=1).astype(jnp.int32)
    chain = jnp.where(pointer >= 0, pointer, slot_ids).astype(jnp.int32)
    for _ in range(panel_width.bit_length()):
        chain = jnp.take(chain, chain).astype(jnp.int32)
    same = pivots[None, :] == pivots[:, None]
    previous = jnp.max(jnp.where(same & earlier, slot_ids[None, :], -1), axis=1).astype(jnp.int32)
    top_source = jnp.where(previous >= 0, jnp.take(chain, jnp.maximum(previous, 0)), pivots).astype(jnp.int32)
    later = slot_ids[None, :] > slot_ids[:, None]
    is_last = jnp.logical_not(jnp.any(same & later, axis=1))
    return top_source, chain, is_last


def global_of_stored(stored):
    return ((stored % ROWS_DEV) // NB * N_PROW + stored // ROWS_DEV) * NB + stored % NB


def stored_of_global(global_rows):
    return ((global_rows // NB) % N_PROW) * ROWS_DEV + (global_rows // (NB * N_PROW)) * NB + global_rows % NB


def reference(a_matrix, l_panel, l_inverse, pivots):
    top_source, moved_source, is_last = swap_plan(pivots, NB)
    targets = jnp.where(is_last & (pivots >= NB), pivots, N).astype(jnp.int32)
    row_source = jnp.arange(N, dtype=jnp.int32).at[targets].set(moved_source, mode="drop")
    row_source = row_source.at[:NB].set(top_source)
    stored = jnp.arange(N, dtype=jnp.int32)
    source_stored = stored_of_global(row_source[global_of_stored(stored)]).astype(jnp.int32)
    swapped = jnp.take(a_matrix, source_stored, axis=0)
    top_rows = jnp.take(a_matrix, stored_of_global(top_source).astype(jnp.int32), axis=0)
    u_block = jnp.dot(l_inverse, top_rows, preferred_element_type=jnp.float32).astype(jnp.bfloat16)
    width_total = a_matrix.shape[1]

    def update_block(pair):
        a_rows, l_rows = pair
        product = jnp.dot(l_rows, u_block, preferred_element_type=jnp.float32)
        return (a_rows.astype(jnp.float32) - product).astype(jnp.bfloat16)

    blocks = lax.map(update_block, (swapped.reshape(N_PROW, ROWS_DEV, width_total), l_panel.reshape(N_PROW, ROWS_DEV, NB)))
    updated = blocks.reshape(N, width_total)
    return updated.at[:NB].set(u_block)
```

```python
import functools

import jax
import jax.numpy as jnp
from jax import lax
from jax.experimental import pallas as pl
from jax.experimental.pallas import tpu as pltpu
from jax.sharding import PartitionSpec as P

MESH = pl.DeviceIdType.MESH
F32 = jnp.float32
BF16 = jnp.bfloat16
CORES = 2


def one_hot(mask):
    return jnp.where(mask, 1.0, 0.0).astype(BF16)


def swap_plan(pv_row):
    nb = pv_row.shape[1]
    slot = lax.broadcasted_iota(jnp.int32, (nb, nb), 0).astype(F32)
    other = lax.broadcasted_iota(jnp.int32, (nb, nb), 1).astype(F32)
    slot_col = lax.broadcasted_iota(jnp.int32, (nb, 1), 0).astype(F32)
    earlier = other < slot
    pv_col = jnp.max(jnp.where(slot == other, pv_row, -1.0), axis=1, keepdims=True)
    pointer = jnp.max(jnp.where((pv_row == slot) & earlier, other, -1.0), axis=1, keepdims=True)
    chain = one_hot(other == jnp.where(pointer >= 0, pointer, slot_col))
    for _ in range((nb - 1).bit_length()):
        chain = jnp.dot(chain, chain, preferred_element_type=F32).astype(BF16)
    same = pv_row == pv_col
    previous = jnp.max(jnp.where(same & earlier, other, -1.0), axis=1, keepdims=True)
    via = jnp.dot(one_hot(other == previous), chain, preferred_element_type=F32)
    via_chain = jnp.max(jnp.where(via > 0.5, other, -1.0), axis=1, keepdims=True)
    top_source = jnp.where(previous >= 0, via_chain, pv_col)
    repeated = jnp.max(jnp.where(same & (slot > other), 1.0, 0.0), axis=0, keepdims=True)
    landing = jnp.where((repeated < 0.5) & (pv_row >= nb), pv_row, -1.0)
    return top_source, chain, landing


def kernel(
    n_prow, n_pcol, chunks,
    a_hbm, l_hbm, inv_hbm, pv_ref, out_hbm,
    a_v, l_full, inv_v, out_v, part, got, mine, tops, origs,
    load_sem, out_sem, own_sem,
    p1_send, p1_recv, p2_send, p2_recv, o1_send, o1_recv, o2_send, o2_recv,
    y_send, y_recv, m_send, m_recv, f_send, f_recv,
):
    rows, width = a_v.shape
    nb = inv_v.shape[0]
    n_red, piece, _ = part.shape
    step = rows // chunks
    n_y = n_pcol // CORES
    me = lax.axis_index("prow")
    col = lax.axis_index("pcol")
    y, core = col // CORES, col % CORES
    mate = y * CORES + (1 - core)

    def y_peer(d):
        return lax.rem(y + d, n_y) * CORES + core

    def y_from(d):
        return lax.rem(y + n_y - d, n_y) * CORES + core

    def to(d):
        return lax.rem(me + d, n_prow)

    def frm(d):
        return lax.rem(me + n_prow - d, n_prow)

    def if_red(index, fn):
        if n_red == n_prow:
            fn()
        else:
            pl.when(index < n_red)(fn)

    l_load = pltpu.make_async_copy(l_hbm, l_full.at[col], load_sem.at[0])
    a_load = pltpu.make_async_copy(a_hbm, a_v, load_sem.at[1])
    inv_load = pltpu.make_async_copy(inv_hbm, inv_v, load_sem.at[2])
    l_load.start()
    a_load.start()
    inv_load.start()

    barrier = pltpu.get_barrier_semaphore()
    for d in range(1, n_prow):
        pl.semaphore_signal(barrier, inc=1, device_id=(to(d), col), device_id_type=MESH)
    for d in range(1, n_y):
        pl.semaphore_signal(barrier, inc=1, device_id=(me, y_peer(d)), device_id_type=MESH)
    pl.semaphore_signal(barrier, inc=1, device_id=(me, mate), device_id_type=MESH)

    top_source, chain, landing = swap_plan(pv_ref[...].astype(F32))

    l_load.wait()
    pl.semaphore_wait(barrier, n_prow - 1 + n_y - 1 + 1)

    def cols(k):
        return pl.ds(k * step, step)

    y_copies = {}
    for k in range(chunks):
        for d in range(1, n_y):
            y_copies[d, k] = pltpu.make_async_remote_copy(
                l_full.at[col, :, cols(k)], l_full.at[col, :, cols(k)],
                y_send.at[d, k], y_recv.at[d, k], device_id=(me, y_peer(d)), device_id_type=MESH)
            y_copies[d, k].start()
    m_copy = pltpu.make_async_remote_copy(
        l_full.at[col], l_full.at[col], m_send, m_recv, device_id=(me, mate), device_id_type=MESH)

    a_load.wait()
    o1_copies = [
        pltpu.make_async_remote_copy(
            a_v.at[pl.ds(d * piece, piece)], origs.at[d], o1_send.at[d], o1_recv,
            device_id=(d, col), device_id_type=MESH)
        for d in range(1, n_red)
    ]
    own_copy = pltpu.make_async_copy(a_v.at[pl.ds(0, piece)], origs.at[0], own_sem)

    @pl.when(me == 0)
    def _():
        for copy in o1_copies:
            copy.start()
        own_copy.start()

    m_copy.start()

    def global_rows(shape, axis, start):
        local = lax.broadcasted_iota(jnp.int32, shape, axis) + start
        return ((local // nb * n_prow + me) * nb + local % nb).astype(F32)

    total = jnp.zeros((nb, width), F32)
    for k in range(chunks):
        pick = one_hot(top_source == global_rows((1, step), 1, k * step))
        total = total + jnp.dot(pick, a_v[pl.ds(k * step, step), :], preferred_element_type=F32)
    part[...] = total.astype(BF16).reshape(n_red, piece, width)

    p1_copies = {}
    for d in range(1, n_prow):
        t = to(d)
        p1_copies[d] = pltpu.make_async_remote_copy(
            part.at[lax.rem(t, n_red)], got.at[d], p1_send.at[d], p1_recv.at[d],
            device_id=(t, col), device_id_type=MESH)
        if_red(t, p1_copies[d].start)

    slot = lax.rem(me, n_red)
    o2_copies, p2_copies = {}, {}
    for d in range(1, n_prow):
        o2_copies[d] = pltpu.make_async_remote_copy(
            origs.at[slot], origs.at[slot], o2_send.at[d], o2_recv.at[d],
            device_id=(to(d), col), device_id_type=MESH)
        p2_copies[d] = pltpu.make_async_remote_copy(
            mine, tops.at[slot], p2_send.at[d], p2_recv.at[d],
            device_id=(to(d), col), device_id_type=MESH)

    @pl.when(me == 0)
    def _():
        own_copy.wait()

    @pl.when((me > 0) & (me < n_red))
    def _():
        o1_copies[0].wait_recv()

    def send_orig():
        for d in range(1, n_prow):
            o2_copies[d].start()

    if_red(me, send_orig)

    def reduce_and_send():
        acc = part[slot].astype(F32)
        for d in range(1, n_prow):
            p1_copies[d].wait_recv()
            acc = acc + got[d].astype(F32)
        mine[...] = acc.astype(BF16)
        tops[slot] = acc.astype(BF16)
        for d in range(1, n_prow):
            p2_copies[d].start()

    if_red(me, reduce_and_send)

    for d in range(1, n_prow):
        if_red(frm(d), o2_copies[d].wait_recv)
    moved = jnp.dot(chain, origs[...].reshape(nb, width), preferred_element_type=F32).astype(BF16)
    moved = jnp.concatenate([moved, jnp.ones((nb, width), BF16)], axis=1)
    for k in range(chunks):
        here = one_hot(landing == global_rows((step, 1), 0, k * step))
        both = jnp.dot(here, moved, preferred_element_type=F32)
        rows_k = pl.ds(k * step, step)
        out_v[rows_k, :] = jnp.where(
            both[:, width:] > 0.5, both[:, :width], a_v[rows_k, :].astype(F32)).astype(BF16)

    for d in range(1, n_prow):
        if_red(frm(d), p2_copies[d].wait_recv)
    inv_load.wait()
    u_block = jnp.dot(
        inv_v[...], tops[...].reshape(nb, width), preferred_element_type=F32).astype(BF16)

    f_copies = {}

    def forward(k):
        for d in range(1, n_y):
            y_copies[d, k].wait_recv()
            src = y_from(d)
            f_copies[d, k] = pltpu.make_async_remote_copy(
                l_full.at[src, :, cols(k)], l_full.at[src, :, cols(k)],
                f_send.at[d, k], f_recv.at[d, k], device_id=(me, mate), device_id_type=MESH)
            f_copies[d, k].start()

    out_copies = []

    def finish(k):
        for d in range(1, n_y):
            f_copies[d, k].wait_recv()
        rows_k = pl.ds(k * step, step)
        panel = l_full[:, :, cols(k)].reshape(nb, step)
        update = lax.dot_general(
            panel, u_block, (((0,), (0,)), ((), ())), preferred_element_type=F32)
        out_v[rows_k, :] = (out_v[rows_k, :].astype(F32) - update).astype(BF16)
        top = min(step, nb - k * step)
        if top > 0:
            @pl.when(me == 0)
            def _():
                out_v[pl.ds(k * step, top), :] = u_block[k * step:k * step + top, :]
        copy = pltpu.make_async_copy(out_v.at[rows_k], out_hbm.at[rows_k], out_sem.at[k])
        copy.start()
        out_copies.append(copy)

    forward(0)
    m_copy.wait_recv()
    for k in range(1, chunks):
        forward(k)
        finish(k - 1)
    finish(chunks - 1)

    @pl.when(me == 0)
    def _():
        for copy in o1_copies:
            copy.wait_send()

    m_copy.wait_send()
    for d in range(1, n_prow):
        if_red(to(d), p1_copies[d].wait_send)

    def drain():
        for d in range(1, n_prow):
            o2_copies[d].wait_send()
            p2_copies[d].wait_send()

    if_red(me, drain)
    for key in y_copies:
        y_copies[key].wait_send()
        f_copies[key].wait_send()
    for copy in out_copies:
        copy.wait()


def body(n_prow, n_pcol, a_matrix, l_panel, l_inverse, pivots):
    rows, width = a_matrix.shape
    nb = l_inverse.shape[0]
    depth = l_panel.shape[1]
    piece = max(16, nb // n_prow)
    n_red = nb // piece
    n_y = n_pcol // CORES
    chunks = min(8, rows // 128)
    dma = pltpu.SemaphoreType.DMA
    return pl.pallas_call(
        functools.partial(kernel, n_prow, n_pcol, chunks),
        out_shape=jax.ShapeDtypeStruct((rows, width), BF16),
        in_specs=[pl.BlockSpec(memory_space=pl.ANY)] * 3 + [pl.BlockSpec(memory_space=pltpu.VMEM)],
        out_specs=pl.BlockSpec(memory_space=pl.ANY),
        scratch_shapes=[
            pltpu.VMEM((rows, width), BF16),
            pltpu.VMEM((n_pcol, depth, rows), BF16),
            pltpu.VMEM((nb, nb), BF16),
            pltpu.VMEM((rows, width), BF16),
            pltpu.VMEM((n_red, piece, width), BF16),
            pltpu.VMEM((n_prow, piece, width), BF16),
            pltpu.VMEM((piece, width), BF16),
            pltpu.VMEM((n_red, piece, width), BF16),
            pltpu.VMEM((n_red, piece, width), BF16),
            dma((3,)), dma((chunks,)), dma,
            dma((n_prow,)), dma((n_prow,)), dma((n_prow,)), dma((n_prow,)),
            dma((n_red,)), dma, dma((n_prow,)), dma((n_prow,)),
            dma((n_y, chunks)), dma((n_y, chunks)), dma, dma,
            dma((n_y, chunks)), dma((n_y, chunks)),
        ],
        compiler_params=pltpu.CompilerParams(
            collective_id=0, has_side_effects=True, vmem_limit_bytes=24 * 2 ** 20),
    )(a_matrix, l_panel.T, l_inverse, pivots.reshape(1, nb))


def solution(mesh):
    n_prow, n_pcol = mesh.shape["prow"], mesh.shape["pcol"]
    in_specs = (P("prow", "pcol"), P("prow", "pcol"), P(), P())
    return jax.shard_map(
        functools.partial(body, n_prow, n_pcol),
        mesh=mesh, in_specs=in_specs, out_specs=P("prow", "pcol"), check_vma=False)
```

```python
import functools

import jax
import jax.numpy as jnp
from jax import lax
from jax.experimental import pallas as pl
from jax.experimental.pallas import tpu as pltpu
from jax.sharding import PartitionSpec as P

MESH = pl.DeviceIdType.MESH
F32 = jnp.float32
BF16 = jnp.bfloat16
CORES = 2


def one_hot(mask):
    return jnp.where(mask, 1.0, 0.0).astype(BF16)


def swap_plan(pv_row):
    nb = pv_row.shape[1]
    slot = lax.broadcasted_iota(jnp.int32, (nb, nb), 0).astype(F32)
    other = lax.broadcasted_iota(jnp.int32, (nb, nb), 1).astype(F32)
    slot_col = lax.broadcasted_iota(jnp.int32, (nb, 1), 0).astype(F32)
    earlier = other < slot
    pv_col = jnp.max(jnp.where(slot == other, pv_row, -1.0), axis=1, keepdims=True)
    pointer = jnp.max(jnp.where((pv_row == slot) & earlier, other, -1.0), axis=1, keepdims=True)
    chain = one_hot(other == jnp.where(pointer >= 0, pointer, slot_col))
    for _ in range((nb - 1).bit_length()):
        chain = jnp.dot(chain, chain, preferred_element_type=F32).astype(BF16)
    same = pv_row == pv_col
    previous = jnp.max(jnp.where(same & earlier, other, -1.0), axis=1, keepdims=True)
    via = jnp.dot(one_hot(other == previous), chain, preferred_element_type=F32)
    via_chain = jnp.max(jnp.where(via > 0.5, other, -1.0), axis=1, keepdims=True)
    top_source = jnp.where(previous >= 0, via_chain, pv_col)
    repeated = jnp.max(jnp.where(same & (slot > other), 1.0, 0.0), axis=0, keepdims=True)
    landing = jnp.where((repeated < 0.5) & (pv_row >= nb), pv_row, -1.0)
    return top_source, chain, landing


def kernel(
    n_prow, n_pcol, chunks,
    a_hbm, l_hbm, inv_hbm, pv_hbm, out_v,
    a_v, l_full, inv_v, pv_ref, part, got, mine, tops, origs,
    load_sem,
    p1_send, p1_recv, p2_send, p2_recv, o1_send, o1_recv, o2_send, o2_recv,
    y_send, y_recv, m_send, m_recv, f_send, f_recv,
):
    rows, width = a_v.shape
    nb = inv_v.shape[0]
    n_red, piece, _ = part.shape
    step = rows // chunks
    n_y = n_pcol // CORES
    me = lax.axis_index("prow")
    col = lax.axis_index("pcol")
    y, core = col // CORES, col % CORES
    mate = y * CORES + (1 - core)

    def y_peer(d):
        return lax.rem(y + d, n_y) * CORES + core

    def y_from(d):
        return lax.rem(y + n_y - d, n_y) * CORES + core

    def to(d):
        return lax.rem(me + d, n_prow)

    def frm(d):
        return lax.rem(me + n_prow - d, n_prow)

    first = (n_prow - n_red) // 2

    def is_red(index):
        return (index >= first) & (index < first + n_red)

    def if_red(index, fn):
        pl.when(is_red(index))(fn)

    def slot_of(index):
        return lax.rem(index + n_prow - first, n_red)

    l_load = pltpu.make_async_copy(l_hbm, l_full.at[col], load_sem.at[0])
    a_load = pltpu.make_async_copy(a_hbm, a_v, load_sem.at[1])
    inv_load = pltpu.make_async_copy(inv_hbm, inv_v, load_sem.at[2])
    pv_load = pltpu.make_async_copy(pv_hbm, pv_ref, load_sem.at[3])
    pv_load.start()
    l_load.start()
    a_load.start()
    inv_load.start()

    barrier = pltpu.get_barrier_semaphore()
    for d in range(1, n_prow):
        @pl.when(is_red(me) | is_red(to(d)))
        def _():
            pl.semaphore_signal(barrier, inc=1, device_id=(to(d), col), device_id_type=MESH)
    for d in range(1, n_y):
        pl.semaphore_signal(barrier, inc=1, device_id=(me, y_peer(d)), device_id_type=MESH)
    pl.semaphore_signal(barrier, inc=1, device_id=(me, mate), device_id_type=MESH)

    pv_load.wait()
    top_source, chain, landing = swap_plan(pv_ref[...].astype(F32))

    l_load.wait()
    pl.semaphore_wait(barrier, n_y + jnp.where(is_red(me), n_prow - 1, n_red))

    def cols(k):
        return pl.ds(k * step, step)

    y_copies = {}
    for k in range(chunks):
        for d in range(1, n_y):
            y_copies[d, k] = pltpu.make_async_remote_copy(
                l_full.at[col, :, cols(k)], l_full.at[col, :, cols(k)],
                y_send.at[d, k], y_recv.at[d, k], device_id=(me, y_peer(d)), device_id_type=MESH)
            y_copies[d, k].start()
    m_copy = pltpu.make_async_remote_copy(
        l_full.at[col], l_full.at[col], m_send, m_recv, device_id=(me, mate), device_id_type=MESH)

    a_load.wait()
    o1_copies = [
        pltpu.make_async_remote_copy(
            a_v.at[pl.ds(d * piece, piece)], origs.at[d], o1_send.at[d], o1_recv,
            device_id=(first + d, col), device_id_type=MESH)
        for d in range(n_red)
    ]

    @pl.when(me == 0)
    def _():
        for copy in o1_copies:
            copy.start()

    m_copy.start()

    def global_rows(shape, axis, start):
        local = lax.broadcasted_iota(jnp.int32, shape, axis) + start
        return ((local // nb * n_prow + me) * nb + local % nb).astype(F32)

    total = jnp.zeros((nb, width), F32)
    for k in range(chunks):
        pick = one_hot(top_source == global_rows((1, step), 1, k * step))
        total = total + jnp.dot(pick, a_v[pl.ds(k * step, step), :], preferred_element_type=F32)
    part[...] = total.astype(BF16).reshape(n_red, piece, width)

    p1_copies = {}
    for d in range(1, n_prow):
        t = to(d)
        p1_copies[d] = pltpu.make_async_remote_copy(
            part.at[slot_of(t)], got.at[d], p1_send.at[d], p1_recv.at[d],
            device_id=(t, col), device_id_type=MESH)
        if_red(t, p1_copies[d].start)

    f_copies = {}

    def forward(k):
        for d in range(1, n_y):
            y_copies[d, k].wait_recv()
            src = y_from(d)
            f_copies[d, k] = pltpu.make_async_remote_copy(
                l_full.at[src, :, cols(k)], l_full.at[src, :, cols(k)],
                f_send.at[d, k], f_recv.at[d, k], device_id=(me, mate), device_id_type=MESH)
            f_copies[d, k].start()

    slot = slot_of(me)
    o2_copies, p2_copies = {}, {}
    for d in range(1, n_prow):
        o2_copies[d] = pltpu.make_async_remote_copy(
            origs.at[slot], origs.at[slot], o2_send.at[d], o2_recv.at[d],
            device_id=(to(d), col), device_id_type=MESH)
        p2_copies[d] = pltpu.make_async_remote_copy(
            mine, tops.at[slot], p2_send.at[d], p2_recv.at[d],
            device_id=(to(d), col), device_id_type=MESH)

    def send_orig():
        o1_copies[0].wait_recv()
        for d in range(1, n_prow):
            o2_copies[d].start()

    if_red(me, send_orig)
    forward(0)
    forward(1)

    def reduce_and_send():
        acc = part[slot].astype(F32)
        for d in range(1, n_prow):
            p1_copies[d].wait_recv()
            acc = acc + got[d].astype(F32)
        mine[...] = acc.astype(BF16)
        tops[slot] = acc.astype(BF16)
        for d in range(1, n_prow):
            p2_copies[d].start()

    if_red(me, reduce_and_send)
    forward(2)

    for d in range(1, n_prow):
        if_red(frm(d), o2_copies[d].wait_recv)
    moved = jnp.dot(chain, origs[...].reshape(nb, width), preferred_element_type=F32).astype(BF16)
    moved = jnp.concatenate([moved, jnp.ones((nb, width), BF16)], axis=1)
    for k in range(chunks):
        here = one_hot(landing == global_rows((step, 1), 0, k * step))
        both = jnp.dot(here, moved, preferred_element_type=F32)
        rows_k = pl.ds(k * step, step)
        out_v[rows_k, :] = jnp.where(
            both[:, width:] > 0.5, both[:, :width], a_v[rows_k, :].astype(F32)).astype(BF16)

    early = min(5, chunks)
    for k in range(3, early):
        forward(k)
    for d in range(1, n_prow):
        if_red(frm(d), p2_copies[d].wait_recv)
    inv_load.wait()
    u_block = jnp.dot(
        inv_v[...], tops[...].reshape(nb, width), preferred_element_type=F32).astype(BF16)

    def finish(k):
        for d in range(1, n_y):
            f_copies[d, k].wait_recv()
        rows_k = pl.ds(k * step, step)
        panel = l_full[:, :, cols(k)].reshape(nb, step)
        update = lax.dot_general(
            panel, u_block, (((0,), (0,)), ((), ())), preferred_element_type=F32)
        out_v[rows_k, :] = (out_v[rows_k, :].astype(F32) - update).astype(BF16)
        top = min(step, nb - k * step)
        if top > 0:
            @pl.when(me == 0)
            def _():
                out_v[pl.ds(k * step, top), :] = u_block[k * step:k * step + top, :]

    m_copy.wait_recv()
    done = 0
    for k in range(early, chunks):
        forward(k)
        while done < k:
            finish(done)
            done += 1
    for k in range(done, chunks):
        finish(k)

    @pl.when(me == 0)
    def _():
        for copy in o1_copies:
            copy.wait_send()

    m_copy.wait_send()
    for d in range(1, n_prow):
        if_red(to(d), p1_copies[d].wait_send)

    def drain():
        for d in range(1, n_prow):
            o2_copies[d].wait_send()
            p2_copies[d].wait_send()

    if_red(me, drain)
    for key in y_copies:
        y_copies[key].wait_send()
        f_copies[key].wait_send()


def hbm(array):
    return pltpu.with_memory_space_constraint(array, pltpu.HBM)


def body(n_prow, n_pcol, a_matrix, l_panel, l_inverse, pivots):
    rows, width = a_matrix.shape
    nb = l_inverse.shape[0]
    depth = l_panel.shape[1]
    n_red = min(n_prow // 2, nb // 16)
    piece = nb // n_red
    n_y = n_pcol // CORES
    chunks = min(8, rows // 128)
    dma = pltpu.SemaphoreType.DMA
    return pl.pallas_call(
        functools.partial(kernel, n_prow, n_pcol, chunks),
        out_shape=jax.ShapeDtypeStruct((rows, width), BF16),
        in_specs=[pl.BlockSpec(memory_space=pl.ANY)] * 4,
        out_specs=pl.BlockSpec(memory_space=pltpu.VMEM),
        scratch_shapes=[
            pltpu.VMEM((rows, width), BF16),
            pltpu.VMEM((n_pcol, depth, rows), BF16),
            pltpu.VMEM((nb, nb), BF16),
            pltpu.VMEM((1, nb), jnp.int32),
            pltpu.VMEM((n_red, piece, width), BF16),
            pltpu.VMEM((n_prow, piece, width), BF16),
            pltpu.VMEM((piece, width), BF16),
            pltpu.VMEM((n_red, piece, width), BF16),
            pltpu.VMEM((n_red, piece, width), BF16),
            dma((4,)),
            dma((n_prow,)), dma((n_prow,)), dma((n_prow,)), dma((n_prow,)),
            dma((n_red,)), dma, dma((n_prow,)), dma((n_prow,)),
            dma((n_y, chunks)), dma((n_y, chunks)), dma, dma,
            dma((n_y, chunks)), dma((n_y, chunks)),
        ],
        compiler_params=pltpu.CompilerParams(
            collective_id=0, has_side_effects=True, vmem_limit_bytes=24 * 2 ** 20),
    )(hbm(a_matrix), hbm(l_panel.T), hbm(l_inverse), hbm(pivots.reshape(1, nb)))


def solution(mesh):
    n_prow, n_pcol = mesh.shape["prow"], mesh.shape["pcol"]
    in_specs = (P("prow", "pcol"), P("prow", "pcol"), P(), P())
    return jax.shard_map(
        functools.partial(body, n_prow, n_pcol),
        mesh=mesh, in_specs=in_specs, out_specs=P("prow", "pcol"), check_vma=False)
```
